32 devices in a mesh: node: 8 (over y, x, core), chip: 4 (over z).
Axes of the slice: x: 2, y: 2, z: 4, core: 2. Of those that a mesh axis runs over, the one named last changes fastest.
Arguments:
- momentum: float32 [32, 128, 512], P(('node', 'chip')), may hold values from -6 to 6
- gradient: bfloat16 [32, 128, 512], P(('node', 'chip')), may hold values from -6 to 6
- indices: int32 [32, 16, 32], P(('node', 'chip')), may hold values from 0 to 4095, as said below
Outputs:
- new_momentum: float32 [32, 128, 512], P(('node', 'chip'))
- update: float32 [128, 512], replicated
The draws below stay inside these ranges and needn't reach their ends.
Inputs may be any that keep to these rules, and one draw needn't show every extreme that they name: `indices`: the 32 entries of each row name distinct coefficients of their span, coefficient (k, l) being k * 64 + l.
All inputs are finite; a program needn't handle non-finite values.
Results may differ from the reference program's by a relative error of at most 0.0029.
Values may be sent and summed in bfloat16 or wider, within the bound.
A program may use at most 64 MiB of HBM per device.

```python
import math
import jax
import jax.numpy as jnp
from jax import lax

KV_WIDTH = 512
ROWS = 128
SPAN = 64
TOPK = 32
SPANS = 16
REPL = 32


def draw_indices(key, part):
    seeds = jax.random.split(key, REPL)

    def draw_one(subkey):
        scores = jax.random.randint(subkey, (SPANS, SPAN * SPAN), 0, 2 ** 18) * (SPAN * SPAN)
        scores = scores + jnp.arange(SPAN * SPAN, dtype=jnp.int32)[None, :]
        unused, picked = lax.top_k(scores, TOPK)
        return picked.astype(jnp.int32)
    return lax.map(draw_one, seeds)


def level_of(own_key, dims, pieces, low, high):
    def one(dim, parts):
        steps = jax.random.uniform(jax.random.fold_in(jax.random.fold_in(own_key, 6), dim), (parts,), jnp.float32, low / len(pieces), high / len(pieces))
        return jnp.repeat(jnp.exp(steps), dims[dim] // parts).reshape((-1,) + (1,) * (len(dims) - dim - 1))

    gain = one(*pieces[0])
    for cut in pieces[1:]:
        gain = gain * one(*cut)
    return gain


def normal_values(rng, shape, spread, reach, pieces=(), held_as=jnp.bfloat16):
    array = jax.random.normal(rng, shape, jnp.float32) * spread
    if len(pieces) > 0:
        array = level_of(rng, shape, pieces, -0.22, 0.18) * array
    return jnp.clip(array, min=-reach, max=reach).astype(held_as)


def setup_inputs(seed: int = 0) -> dict:
    key_list = jax.random.split(jax.random.key(seed), 4)
    return {
        "momentum": normal_values(key_list[0], (REPL, ROWS, KV_WIDTH), 1.0, 6.0, ((0, 32),), jnp.float32),
        "gradient": normal_values(key_list[1], (REPL, ROWS, KV_WIDTH), 1.0, 6.0, ((0, 32),)),
        "indices": draw_indices(jax.random.fold_in(key_list[3], 71), 0),
    }


def dct_table(edge_len):
    orders = jnp.arange(edge_len, dtype=jnp.float32)
    wave_no = orders[:, None]
    cell_no = orders[None, :]
    factor = jnp.where(wave_no == 0.0, math.sqrt(1.0 / edge_len), math.sqrt(2.0 / edge_len))
    return factor * jnp.cos(math.pi * (2.0 * cell_no + 1.0) * wave_no / (2.0 * edge_len))

def forward(grid_field, cosines, edge_len):
    row_blocks = grid_field.shape[0] // edge_len
    col_blocks = grid_field.shape[1] // edge_len
    blocks = grid_field.reshape(row_blocks, edge_len, col_blocks, edge_len).transpose(0, 2, 1, 3)
    coeffs = jnp.einsum('kn,abnm,lm->abkl', cosines, blocks, cosines, precision=lax.Precision.HIGHEST)
    return coeffs.reshape(row_blocks * col_blocks, edge_len * edge_len)

def inverse_blocks(coeffs, cosines, edge_len):
    blocks = coeffs.reshape(coeffs.shape[0], edge_len, edge_len)
    return jnp.einsum('kn,ckl,lm->cnm', cosines, blocks, cosines, precision=lax.Precision.HIGHEST)

def place_blocks(blocks, row_count, col_count, edge_len):
    shaped = blocks.reshape(row_count // edge_len, col_count // edge_len, edge_len, edge_len)
    return shaped.transpose(0, 2, 1, 3).reshape(row_count, col_count)

def normalized(blocks):
    energy = lax.optimization_barrier(jnp.mean(blocks * blocks, axis=(1, 2), keepdims=True))
    return blocks / jnp.sqrt(energy + 1.0)

def add_entries(totals, picked, slots):
    span_ids = jnp.broadcast_to(jnp.arange(slots.shape[-2], dtype=jnp.int32)[:, None], slots.shape)
    return totals.at[span_ids, slots].add(picked.astype(jnp.float32))

def reference(momentum, gradient, indices):
    cosines = dct_table(SPAN)
    n_spans = ROWS // SPAN * (KV_WIDTH // SPAN)

    def replica_step(totals, inputs_row):
        moment, grad_row, slots = inputs_row
        blended = 0.9 * moment + grad_row.astype(jnp.float32)
        coeffs = forward(blended, cosines, SPAN)
        picked = jnp.take_along_axis(coeffs, slots, axis=1).astype(jnp.bfloat16)
        sparse = add_entries(jnp.zeros_like(coeffs), picked, slots)
        own_part = place_blocks(inverse_blocks(sparse, cosines, SPAN), ROWS, KV_WIDTH, SPAN)
        return (totals + sparse, blended - own_part)
    start_sum = jnp.zeros((n_spans, SPAN * SPAN), jnp.float32)
    totals, new_momentum = lax.scan(replica_step, start_sum, (momentum, gradient, indices))
    update = place_blocks(normalized(inverse_blocks(totals, cosines, SPAN)), ROWS, KV_WIDTH, SPAN)
    return (new_momentum, update)
```

```python
import functools
import math

import jax
import jax.numpy as jnp
import numpy as np
from jax import lax
from jax.experimental import pallas as pl
from jax.experimental.pallas import tpu as pltpu
from jax.sharding import PartitionSpec as P

SPAN = 64
LANES = 128
MESH = pl.DeviceIdType.MESH
F32 = jnp.float32
BF16 = jnp.bfloat16


def cosine_blocks(copies):
    orders = np.arange(SPAN, dtype=np.float64)
    wave, cell = orders[:, None], orders[None, :]
    factor = np.where(wave == 0, math.sqrt(1 / SPAN), math.sqrt(2 / SPAN))
    table = factor * np.cos(math.pi * (2 * cell + 1) * wave / (2 * SPAN))
    full = np.kron(np.eye(copies), table)
    high = full.astype(BF16)
    low = (full - high.astype(np.float64)).astype(BF16)
    return np.stack([high.T, low.T, high, low])


def halves(x):
    high = x.astype(BF16)
    return high, (x - high.astype(F32)).astype(BF16)


def mm(a, b):
    return lax.dot_general(a, b, (((1,), (0,)), ((), ())), preferred_element_type=F32)


def mm_nt(a, b):
    return lax.dot_general(a, b, (((1,), (1,)), ((), ())), preferred_element_type=F32)


def both_sides(blocks, left, right, exact):
    outs = []
    for x in blocks:
        if exact:
            y = mm(x, right[0]) + mm(x, right[1])
        else:
            high, low = halves(x)
            y = mm(high, right[0]) + (mm(low, right[0]) + mm(high, right[1]))
        high, low = halves(y)
        outs.append(mm(left[0], high) + (mm(left[0], low) + mm(left[1], high)))
    return outs


def kernel(
    nodes, chips, topk, mom_hbm, grad_hbm, idx_hbm, cos_hbm, new_hbm, upd_hbm,
    mom, grad, idx, cos, new_out, upd, box, recv, acc, in_sem, out_sem, send_sem, recv_sem,
):
    node, chip = lax.axis_index("node"), lax.axis_index("chip")
    count = nodes * chips
    rows, cols = mom.shape
    per = LANES // topk
    wide = per * SPAN
    groups = idx.shape[0] // per
    strips = cols // wide
    used = 3 * groups

    loads = [
        pltpu.make_async_copy(src, dst, in_sem.at[i])
        for i, (src, dst) in enumerate(
            ((idx_hbm.at[0], idx), (mom_hbm.at[0], mom), (grad_hbm.at[0], grad), (cos_hbm, cos))
        )
    ]
    for load in loads:
        load.start()

    barrier = pltpu.get_barrier_semaphore()

    def peers(visit):
        def one(off, i):
            to_node = lax.rem(node + i, nodes)
            to_chip = lax.rem(chip + off, chips)
            visit(off, {"node": to_node, "chip": to_chip})

        order = sorted(range(chips), key=lambda o: -min(o, chips - o))
        for off in order:
            first = 1 if off == 0 else 0
            if nodes <= 8:
                for i in range(first, nodes):
                    one(off, i)
            else:
                pl.loop(first, nodes)(functools.partial(one, off))

    peers(lambda off, to: pl.semaphore_signal(barrier, inc=1, device_id=to, device_id_type=MESH))

    loads[0].wait()
    slots = idx[...]
    spans = slots.shape[0]
    lane = lax.broadcasted_iota(jnp.int32, (spans, LANES), 1)
    place = lax.broadcasted_iota(jnp.int32, (spans, LANES), 0) % per
    spread = jnp.concatenate([slots] * per, axis=1)
    spread = jnp.where(lane // topk == place, spread + place * (SPAN * SPAN), 0)
    lists = [
        jnp.sum(spread[g * per:(g + 1) * per], axis=0, keepdims=True) for g in range(groups)
    ]
    wave = [(x // SPAN) % SPAN for x in lists]
    wide_pos = [(x // (SPAN * SPAN)) * SPAN + x % SPAN for x in lists]
    tall_iota = lax.broadcasted_iota(jnp.int32, (SPAN, LANES), 0)
    wide_iota = lax.broadcasted_iota(jnp.int32, (wide, LANES), 0)
    wave_hot = [(tall_iota == w).astype(F32) for w in wave]
    wide_hot = [(wide_iota == w).astype(F32).astype(BF16) for w in wide_pos]

    for load in loads[1:]:
        load.wait()
    blended = 0.9 * mom[...] + grad[...].astype(F32)
    fwd_right = (cos[0], cos[1])
    fwd_left = (cos[2, :rows, :rows], cos[3, :rows, :rows])
    inv_right = (cos[2], cos[3])
    inv_left = (cos[0, :rows, :rows], cos[1, :rows, :rows])
    strip = lambda x: [x[:, s * wide:(s + 1) * wide] for s in range(strips)]
    coeffs = [x.astype(BF16) for x in both_sides(strip(blended), fwd_left, fwd_right, False)]

    def part(g):
        a, s = g // strips, g % strips
        return a, s

    picked = []
    for g in range(groups):
        a, s = part(g)
        own = coeffs[s][a * SPAN:(a + 1) * SPAN]
        picked.append(jnp.sum(mm(own, wide_hot[g]) * wave_hot[g], axis=0, keepdims=True))
    payload = jnp.concatenate(
        picked + [w.astype(F32) for w in wave] + [w.astype(F32) for w in wide_pos], axis=0
    ).astype(BF16)
    me = chip * nodes + node
    box[...] = payload
    recv[me] = payload

    pl.semaphore_wait(barrier, count - 1)
    peers(
        lambda off, to: pltpu.make_async_remote_copy(
            src_ref=box,
            dst_ref=recv.at[me],
            send_sem=send_sem,
            recv_sem=recv_sem.at[off],
            device_id=to,
            device_id_type=MESH,
        ).start()
    )

    sparse_rows = [[None] * strips for _ in range(rows // SPAN)]
    for g in range(groups):
        a, s = part(g)
        mask = mm_nt(wave_hot[g].astype(BF16), wide_hot[g])
        own = coeffs[s][a * SPAN:(a + 1) * SPAN].astype(F32)
        sparse_rows[a][s] = (mask * own).astype(BF16)
    sparse = [
        jnp.concatenate([row[s] for row in sparse_rows], axis=0) for s in range(strips)
    ]
    own_part = both_sides(sparse, inv_left, inv_right, True)
    for s in range(strips):
        cut = slice(s * wide, (s + 1) * wide)
        new_out[:, cut] = blended[:, cut] - own_part[s]
    store_new = pltpu.make_async_copy(new_out, new_hbm.at[0], out_sem.at[0])
    store_new.start()

    acc[...] = jnp.zeros_like(acc)
    batch = math.gcd(nodes, 8)

    def decode(start):
        block = recv[pl.ds(start, batch)].astype(F32)
        for g in range(groups):
            left, right = [], []
            for i in range(batch):
                val = block[i, g:g + 1]
                row = block[i, groups + g:groups + g + 1].astype(jnp.int32)
                col = block[i, 2 * groups + g:2 * groups + g + 1].astype(jnp.int32)
                left.append(jnp.where(tall_iota == row, val, 0.0).astype(BF16))
                right.append((wide_iota == col).astype(F32).astype(BF16))
            a, s = part(g)
            acc[pl.ds(a * SPAN, SPAN), pl.ds(s * wide, wide)] += mm_nt(
                jnp.concatenate(left, axis=1), jnp.concatenate(right, axis=1)
            )

    for off in sorted(range(chips), key=lambda o: min(o, chips - o)):
        source = lax.rem(chip + chips - off, chips) * nodes
        landed = recv.at[pl.ds(source, nodes - 1 if off == 0 else nodes)]
        pltpu.make_async_copy(landed, landed, recv_sem.at[off]).wait()
        if nodes == batch:
            decode(source)
        else:
            pl.loop(0, nodes // batch)(lambda i: decode(source + i * batch))

    totals = strip(acc[...])
    field = both_sides(totals, inv_left, inv_right, False)
    same = (
        lax.broadcasted_iota(jnp.int32, (wide, wide), 0) // SPAN
        == lax.broadcasted_iota(jnp.int32, (wide, wide), 1) // SPAN
    ).astype(F32).astype(BF16)
    for s in range(strips):
        for a in range(rows // SPAN):
            band = slice(a * SPAN, (a + 1) * SPAN)
            power = totals[s][band] * totals[s][band]
            power = jnp.sum(power.reshape(SPAN // 8, 8, wide), axis=0)
            high, low = halves(power)
            energy = jnp.sum(mm(high, same) + mm(low, same), axis=0, keepdims=True)
            scale = 1.0 / jnp.sqrt(energy * (1.0 / (SPAN * SPAN)) + 1.0)
            upd[band, s * wide:(s + 1) * wide] = field[s][band] * scale
    store_upd = pltpu.make_async_copy(upd, upd_hbm, out_sem.at[1])
    store_upd.start()

    sent = recv.at[pl.ds(0, count - 1)]
    pltpu.make_async_copy(sent, sent, send_sem).wait()
    store_new.wait()
    store_upd.wait()


def solution(mesh):
    nodes, chips = mesh.shape["node"], mesh.shape["chip"]

    def step(momentum, gradient, indices):
        _, rows, cols = momentum.shape
        spans, topk = indices.shape[1:]
        per = LANES // topk
        wide = per * SPAN
        used = 3 * (spans // per)
        cosines = jnp.asarray(cosine_blocks(per))
        hbm = pl.BlockSpec(memory_space=pl.ANY)
        return tuple(pl.pallas_call(
            functools.partial(kernel, nodes, chips, topk),
            out_shape=(
                jax.ShapeDtypeStruct((1, rows, cols), F32),
                jax.ShapeDtypeStruct((rows, cols), F32),
            ),
            in_specs=[hbm] * 4,
            out_specs=(hbm, hbm),
            scratch_shapes=[
                pltpu.VMEM((rows, cols), F32),
                pltpu.VMEM((rows, cols), BF16),
                pltpu.VMEM((spans, topk), jnp.int32),
                pltpu.VMEM((4, wide, wide), BF16),
                pltpu.VMEM((rows, cols), F32),
                pltpu.VMEM((rows, cols), F32),
                pltpu.VMEM((used, LANES), BF16),
                pltpu.VMEM((nodes * chips, used, LANES), BF16),
                pltpu.VMEM((rows, cols), F32),
                pltpu.SemaphoreType.DMA((4,)),
                pltpu.SemaphoreType.DMA((2,)),
                pltpu.SemaphoreType.DMA,
                pltpu.SemaphoreType.DMA((chips,)),
            ],
            compiler_params=pltpu.CompilerParams(collective_id=0, has_side_effects=True),
        )(momentum, gradient, indices, cosines))

    return jax.shard_map(
        step,
        mesh=mesh,
        in_specs=(P(("node", "chip"), None, None),) * 3,
        out_specs=(P(("node", "chip"), None, None), P()),
        check_vma=False,
    )
```

```python
import functools
import math

import jax
import jax.numpy as jnp
import numpy as np
from jax import lax
from jax.experimental import pallas as pl
from jax.experimental.pallas import tpu as pltpu
from jax.sharding import PartitionSpec as P

SPAN = 64
LANES = 128
MESH = pl.DeviceIdType.MESH
F32 = jnp.float32
BF16 = jnp.bfloat16


def cosine_blocks(copies):
    orders = np.arange(SPAN, dtype=np.float64)
    wave, cell = orders[:, None], orders[None, :]
    factor = np.where(wave == 0, math.sqrt(1 / SPAN), math.sqrt(2 / SPAN))
    table = factor * np.cos(math.pi * (2 * cell + 1) * wave / (2 * SPAN))
    full = np.kron(np.eye(copies), table)
    high = full.astype(BF16)
    low = (full - high.astype(np.float64)).astype(BF16)
    return np.stack([high.T, low.T, high, low])


def halves(x):
    high = x.astype(BF16)
    return high, (x - high.astype(F32)).astype(BF16)


def mm(a, b):
    return lax.dot_general(a, b, (((1,), (0,)), ((), ())), preferred_element_type=F32)


def mm_nt(a, b):
    return lax.dot_general(a, b, (((1,), (1,)), ((), ())), preferred_element_type=F32)


def both_sides(blocks, left, right, exact):
    outs = []
    for x in blocks:
        if exact:
            y = mm(x, right[0]) + mm(x, right[1])
        else:
            high, low = halves(x)
            y = mm(high, right[0]) + (mm(low, right[0]) + mm(high, right[1]))
        high, low = halves(y)
        outs.append(mm(left[0], high) + (mm(left[0], low) + mm(left[1], high)))
    return outs


def kernel(
    nodes, chips, topk, mom_hbm, grad_hbm, idx_hbm, cos_hbm, new_out, acc, cos,
    mom, grad, idx, box, recv, in_sem, send_sem, recv_sem,
):
    node, chip = lax.axis_index("node"), lax.axis_index("chip")
    count = nodes * chips
    rows, cols = mom.shape
    per = LANES // topk
    wide = per * SPAN
    groups = idx.shape[0] // per
    strips = cols // wide
    used = 3 * groups

    loads = [
        pltpu.make_async_copy(src, dst, in_sem.at[i])
        for i, (src, dst) in enumerate(
            ((idx_hbm.at[0], idx), (mom_hbm.at[0], mom), (grad_hbm.at[0], grad), (cos_hbm, cos))
        )
    ]
    for load in loads:
        load.start()

    barrier = pltpu.get_barrier_semaphore()

    def peers(visit):
        def one(off, i):
            to_node = lax.rem(node + i, nodes)
            to_chip = lax.rem(chip + off, chips)
            visit(off, {"node": to_node, "chip": to_chip})

        order = sorted(range(chips), key=lambda o: -min(o, chips - o))
        for off in order:
            first = 1 if off == 0 else 0
            if nodes <= 8:
                for i in range(first, nodes):
                    one(off, i)
            else:
                pl.loop(first, nodes)(functools.partial(one, off))

    peers(lambda off, to: pl.semaphore_signal(barrier, inc=1, device_id=to, device_id_type=MESH))

    loads[0].wait()
    slots = idx[...]
    spans = slots.shape[0]
    lane = lax.broadcasted_iota(jnp.int32, (spans, LANES), 1)
    place = lax.broadcasted_iota(jnp.int32, (spans, LANES), 0) % per
    spread = jnp.concatenate([slots] * per, axis=1)
    spread = jnp.where(lane // topk == place, spread + place * (SPAN * SPAN), 0)
    lists = [
        jnp.sum(spread[g * per:(g + 1) * per], axis=0, keepdims=True) for g in range(groups)
    ]
    wave = [(x // SPAN) % SPAN for x in lists]
    wide_pos = [(x // (SPAN * SPAN)) * SPAN + x % SPAN for x in lists]
    tall_iota = lax.broadcasted_iota(jnp.int32, (SPAN, LANES), 0)
    wide_iota = lax.broadcasted_iota(jnp.int32, (wide, LANES), 0)
    wave_hot = [(tall_iota == w).astype(F32) for w in wave]
    wide_hot = [(wide_iota == w).astype(F32).astype(BF16) for w in wide_pos]

    for load in loads[1:]:
        load.wait()
    blended = 0.9 * mom[...] + grad[...].astype(F32)
    fwd_right = (cos[0], cos[1])
    fwd_left = (cos[2, :rows, :rows], cos[3, :rows, :rows])
    inv_right = (cos[2], cos[3])
    inv_left = (cos[0, :rows, :rows], cos[1, :rows, :rows])
    strip = lambda x: [x[:, s * wide:(s + 1) * wide] for s in range(strips)]
    coeffs = [x.astype(BF16) for x in both_sides(strip(blended), fwd_left, fwd_right, False)]

    def part(g):
        a, s = g // strips, g % strips
        return a, s

    picked = []
    for g in range(groups):
        a, s = part(g)
        own = coeffs[s][a * SPAN:(a + 1) * SPAN]
        picked.append(jnp.sum(mm(own, wide_hot[g]) * wave_hot[g], axis=0, keepdims=True))
    payload = jnp.concatenate(
        picked + [w.astype(F32) for w in wave] + [w.astype(F32) for w in wide_pos], axis=0
    ).astype(BF16)
    me = chip * nodes + node
    box[...] = payload
    recv[me] = payload

    pl.semaphore_wait(barrier, count - 1)
    peers(
        lambda off, to: pltpu.make_async_remote_copy(
            src_ref=box,
            dst_ref=recv.at[me],
            send_sem=send_sem,
            recv_sem=recv_sem.at[off],
            device_id=to,
            device_id_type=MESH,
        ).start()
    )

    sparse_rows = [[None] * strips for _ in range(rows // SPAN)]
    for g in range(groups):
        a, s = part(g)
        mask = mm_nt(wave_hot[g].astype(BF16), wide_hot[g])
        own = coeffs[s][a * SPAN:(a + 1) * SPAN].astype(F32)
        sparse_rows[a][s] = (mask * own).astype(BF16)
    sparse = [
        jnp.concatenate([row[s] for row in sparse_rows], axis=0) for s in range(strips)
    ]
    own_part = both_sides(sparse, inv_left, inv_right, True)
    for s in range(strips):
        cut = slice(s * wide, (s + 1) * wide)
        new_out[:, cut] = blended[:, cut] - own_part[s]

    acc[...] = jnp.zeros_like(acc)
    batch = math.gcd(nodes, 8)

    def decode(start):
        block = recv[pl.ds(start, batch)].astype(F32)
        for g in range(groups):
            left, right = [], []
            for i in range(batch):
                val = block[i, g:g + 1]
                row = block[i, groups + g:groups + g + 1].astype(jnp.int32)
                col = block[i, 2 * groups + g:2 * groups + g + 1].astype(jnp.int32)
                left.append(jnp.where(tall_iota == row, val, 0.0).astype(BF16))
                right.append((wide_iota == col).astype(F32).astype(BF16))
            a, s = part(g)
            acc[pl.ds(a * SPAN, SPAN), pl.ds(s * wide, wide)] += mm_nt(
                jnp.concatenate(left, axis=1), jnp.concatenate(right, axis=1)
            )

    for off in sorted(range(chips), key=lambda o: min(o, chips - o)):
        source = lax.rem(chip + chips - off, chips) * nodes
        landed = recv.at[pl.ds(source, nodes - 1 if off == 0 else nodes)]
        pltpu.make_async_copy(landed, landed, recv_sem.at[off]).wait()
        if nodes == batch:
            decode(source)
        else:
            pl.loop(0, nodes // batch)(lambda i: decode(source + i * batch))

    sent = recv.at[pl.ds(0, count - 1)]
    pltpu.make_async_copy(sent, sent, send_sem).wait()


def finish(new_in, acc, cos, new_hbm, upd_hbm, upd, sem):
    store_new = pltpu.make_async_copy(new_in, new_hbm.at[0], sem.at[0])
    store_new.start()
    rows, cols = acc.shape
    wide = cos.shape[-1]
    strips = cols // wide
    totals = [acc[:, s * wide:(s + 1) * wide] for s in range(strips)]
    same = (
        lax.broadcasted_iota(jnp.int32, (wide, wide), 0) // SPAN
        == lax.broadcasted_iota(jnp.int32, (wide, wide), 1) // SPAN
    ).astype(F32).astype(BF16)
    field = both_sides(
        totals,
        (cos[0, :rows, :rows], cos[1, :rows, :rows]),
        (cos[2], cos[3]),
        False,
    )
    for s in range(strips):
        for a in range(rows // SPAN):
            band = slice(a * SPAN, (a + 1) * SPAN)
            power = totals[s][band] * totals[s][band]
            power = jnp.sum(power.reshape(SPAN // 8, 8, wide), axis=0)
            high, low = halves(power)
            energy = jnp.sum(mm(high, same) + mm(low, same), axis=0, keepdims=True)
            scale = 1.0 / jnp.sqrt(energy * (1.0 / (SPAN * SPAN)) + 1.0)
            upd[band, s * wide:(s + 1) * wide] = field[s][band] * scale
    store_upd = pltpu.make_async_copy(upd, upd_hbm, sem.at[1])
    store_upd.start()
    store_new.wait()
    store_upd.wait()


def solution(mesh):
    nodes, chips = mesh.shape["node"], mesh.shape["chip"]

    def step(momentum, gradient, indices):
        _, rows, cols = momentum.shape
        spans, topk = indices.shape[1:]
        per = LANES // topk
        wide = per * SPAN
        used = 3 * (spans // per)
        cosines = jnp.asarray(cosine_blocks(per))
        hbm = pl.BlockSpec(memory_space=pltpu.HBM)
        vmem = pl.BlockSpec(memory_space=pltpu.VMEM)
        new_momentum, totals, tables = pl.pallas_call(
            functools.partial(kernel, nodes, chips, topk),
            out_shape=(
                pltpu.VMEM((rows, cols), F32),
                pltpu.VMEM((rows, cols), F32),
                pltpu.VMEM((4, wide, wide), BF16),
            ),
            in_specs=[hbm] * 4,
            out_specs=(vmem, vmem, vmem),
            scratch_shapes=[
                pltpu.VMEM((rows, cols), F32),
                pltpu.VMEM((rows, cols), BF16),
                pltpu.VMEM((spans, topk), jnp.int32),
                pltpu.VMEM((used, LANES), BF16),
                pltpu.VMEM((nodes * chips, used, LANES), BF16),
                pltpu.SemaphoreType.DMA((4,)),
                pltpu.SemaphoreType.DMA,
                pltpu.SemaphoreType.DMA((chips,)),
            ],
            compiler_params=pltpu.CompilerParams(
                collective_id=0, has_side_effects=True, vmem_limit_bytes=24 * 2**20
            ),
        )(*(pltpu.with_memory_space_constraint(x, pltpu.HBM) for x in (momentum, gradient, indices, cosines)))
        return tuple(pl.pallas_call(
            finish,
            out_shape=(
                jax.ShapeDtypeStruct((1, rows, cols), F32),
                jax.ShapeDtypeStruct((rows, cols), F32),
            ),
            in_specs=[vmem, vmem, vmem],
            out_specs=(hbm, hbm),
            scratch_shapes=[
                pltpu.VMEM((rows, cols), F32),
                pltpu.SemaphoreType.DMA((2,)),
            ],
            compiler_params=pltpu.CompilerParams(vmem_limit_bytes=24 * 2**20),
        )(new_momentum, totals, tables))

    return jax.shard_map(
        step,
        mesh=mesh,
        in_specs=(P(("node", "chip"), None, None),) * 3,
        out_specs=(P(("node", "chip"), None, None), P()),
        check_vma=False,
    )
```

```python
import functools
import math

import jax
import jax.numpy as jnp
import numpy as np
from jax import lax
from jax.experimental import pallas as pl
from jax.experimental.pallas import tpu as pltpu
from jax.sharding import PartitionSpec as P

SPAN = 64
LANES = 128
MESH = pl.DeviceIdType.MESH
F32 = jnp.float32
BF16 = jnp.bfloat16


def cosine_blocks(copies):
    orders = np.arange(SPAN, dtype=np.float64)
    wave, cell = orders[:, None], orders[None, :]
    factor = np.where(wave == 0, math.sqrt(1 / SPAN), math.sqrt(2 / SPAN))
    table = factor * np.cos(math.pi * (2 * cell + 1) * wave / (2 * SPAN))
    full = np.kron(np.eye(copies), table)
    high = full.astype(BF16)
    low = (full - high.astype(np.float64)).astype(BF16)
    return np.stack([high.T, low.T, high, low])


def halves(x):
    high = x.astype(BF16)
    return high, (x - high.astype(F32)).astype(BF16)


def mm(a, b):
    return lax.dot_general(a, b, (((1,), (0,)), ((), ())), preferred_element_type=F32)


def mm_nt(a, b):
    return lax.dot_general(a, b, (((1,), (1,)), ((), ())), preferred_element_type=F32)


def both_sides(blocks, left, right):
    outs = []
    for x in blocks:
        high, low = halves(x)
        y = mm(high, right[0]) + (mm(low, right[0]) + mm(high, right[1]))
        high, low = halves(y)
        outs.append(mm(left[0], high) + (mm(left[0], low) + mm(left[1], high)))
    return outs


def kernel(
    nodes, chips, topk, mom_hbm, grad_hbm, idx_hbm, cos_hbm, new_out, acc, cos,
    mom, grad, idx, box, recv, in_sem, send_sem, recv_sem,
):
    node, chip = lax.axis_index("node"), lax.axis_index("chip")
    count = nodes * chips
    rows, cols = mom.shape
    per = LANES // topk
    wide = per * SPAN
    groups = idx.shape[0] // per
    strips = cols // wide
    used = 3 * groups

    loads = [
        pltpu.make_async_copy(src, dst, in_sem.at[i])
        for i, (src, dst) in enumerate(
            (
                (idx_hbm.at[0], idx),
                (cos_hbm.at[pl.ds(0, 2)], cos.at[pl.ds(0, 2)]),
                (mom_hbm.at[0], mom),
                (grad_hbm.at[0], grad),
                (cos_hbm.at[pl.ds(2, 2)], cos.at[pl.ds(2, 2)]),
            )
        )
    ]
    for load in loads:
        load.start()

    barrier = pltpu.get_barrier_semaphore()

    high_side = 2 * chip >= chips

    def plane(t):
        up = t + (chip <= t).astype(jnp.int32)
        down = chips - 1 - t
        return jnp.where(high_side, up, down - (down <= chip).astype(jnp.int32))

    def peers(visit):
        def one(to_chip, base, i):
            visit({"node": lax.rem(base + i, nodes), "chip": to_chip})

        for t in range(chips):
            own = t == chips - 1
            go = functools.partial(one, *((chip, node) if own else (plane(t), nodes - 1 - node)))
            if nodes <= 8:
                for i in range(1 if own else 0, nodes):
                    go(i)
            else:
                pl.loop(1 if own else 0, nodes)(go)

    peers(lambda to: pl.semaphore_signal(barrier, inc=1, device_id=to, device_id_type=MESH))

    loads[0].wait()
    slots = idx[...]
    spans = slots.shape[0]
    lane = lax.broadcasted_iota(jnp.int32, (spans, LANES), 1)
    place = lax.broadcasted_iota(jnp.int32, (spans, LANES), 0) % per
    spread = jnp.concatenate([slots] * per, axis=1)
    spread = jnp.where(lane // topk == place, spread + place * (SPAN * SPAN), 0)
    lists = [
        jnp.sum(spread[g * per:(g + 1) * per], axis=0, keepdims=True) for g in range(groups)
    ]
    wave = [(x // SPAN) % SPAN for x in lists]
    wide_pos = [(x // (SPAN * SPAN)) * SPAN + x % SPAN for x in lists]
    tall_iota = lax.broadcasted_iota(jnp.int32, (SPAN, LANES), 0)
    wide_iota = lax.broadcasted_iota(jnp.int32, (wide, LANES), 0)
    wave_hot = [(tall_iota == w).astype(F32).astype(BF16) for w in wave]
    wide_hot = [(wide_iota == w).astype(F32).astype(BF16) for w in wide_pos]

    loads[1].wait()
    tall_cos = [
        mm(cos[0, :SPAN, :SPAN], hot) + mm(cos[1, :SPAN, :SPAN], hot) for hot in wave_hot
    ]
    wide_high = [mm(cos[0], hot).astype(BF16) for hot in wide_hot]
    wide_low = [mm(cos[1], hot).astype(BF16) for hot in wide_hot]

    loads[2].wait()
    loads[3].wait()
    blended = 0.9 * mom[...] + grad[...].astype(F32)

    def part(g):
        a, s = g // strips, g % strips
        return a, s

    def region(g):
        a, s = part(g)
        return slice(a * SPAN, (a + 1) * SPAN), slice(s * wide, (s + 1) * wide)

    picked = []
    for g in range(groups):
        high, low = halves(blended[region(g)])
        sums = mm(high, wide_high[g]) + (mm(low, wide_high[g]) + mm(high, wide_low[g]))
        picked.append(jnp.sum(sums * tall_cos[g], axis=0, keepdims=True))
    payload = jnp.concatenate(
        picked + [w.astype(F32) for w in wave] + [w.astype(F32) for w in wide_pos], axis=0
    ).astype(BF16)
    me = chip * nodes + node
    box[...] = payload
    recv[me] = payload

    pl.semaphore_wait(barrier, count - 1)
    peers(
        lambda to: pltpu.make_async_remote_copy(
            src_ref=box,
            dst_ref=recv.at[me],
            send_sem=send_sem,
            recv_sem=recv_sem.at[chip],
            device_id=to,
            device_id_type=MESH,
        ).start()
    )

    for g in range(groups):
        sent_value = picked[g].astype(BF16).astype(F32)
        high, low = halves(tall_cos[g] * sent_value)
        own_part = mm_nt(high, wide_high[g]) + (
            mm_nt(low, wide_high[g]) + mm_nt(high, wide_low[g])
        )
        new_out[region(g)] = blended[region(g)] - own_part

    acc[...] = jnp.zeros_like(acc)
    batch = math.gcd(nodes, 8)

    def decode(start):
        block = recv[pl.ds(start, batch)].astype(F32)
        for g in range(groups):
            left, right = [], []
            for i in range(batch):
                val = block[i, g:g + 1]
                row = block[i, groups + g:groups + g + 1].astype(jnp.int32)
                col = block[i, 2 * groups + g:2 * groups + g + 1].astype(jnp.int32)
                left.append(jnp.where(tall_iota == row, val, 0.0).astype(BF16))
                right.append((wide_iota == col).astype(F32).astype(BF16))
            a, s = part(g)
            acc[pl.ds(a * SPAN, SPAN), pl.ds(s * wide, wide)] += mm_nt(
                jnp.concatenate(left, axis=1), jnp.concatenate(right, axis=1)
            )

    for t in reversed(range(chips)):
        source = chip if t == chips - 1 else plane(t)
        first = source * nodes
        landed = recv.at[pl.ds(first, nodes - 1 if t == chips - 1 else nodes)]
        pltpu.make_async_copy(landed, landed, recv_sem.at[source]).wait()
        if nodes == batch:
            decode(first)
        else:
            pl.loop(0, nodes // batch)(lambda i: decode(first + i * batch))

    loads[4].wait()
    sent = recv.at[pl.ds(0, count - 1)]
    pltpu.make_async_copy(sent, sent, send_sem).wait()


def finish(new_in, acc, cos, new_hbm, upd_hbm, upd, sem):
    store_new = pltpu.make_async_copy(new_in, new_hbm.at[0], sem.at[0])
    store_new.start()
    rows, cols = acc.shape
    wide = cos.shape[-1]
    strips = cols // wide
    totals = [acc[:, s * wide:(s + 1) * wide] for s in range(strips)]
    same = (
        lax.broadcasted_iota(jnp.int32, (wide, wide), 0) // SPAN
        == lax.broadcasted_iota(jnp.int32, (wide, wide), 1) // SPAN
    ).astype(F32).astype(BF16)
    field = both_sides(
        totals,
        (cos[0, :rows, :rows], cos[1, :rows, :rows]),
        (cos[2], cos[3]),
    )
    for s in range(strips):
        for a in range(rows // SPAN):
            band = slice(a * SPAN, (a + 1) * SPAN)
            power = totals[s][band] * totals[s][band]
            power = jnp.sum(power.reshape(SPAN // 8, 8, wide), axis=0)
            high, low = halves(power)
            energy = jnp.sum(mm(high, same) + mm(low, same), axis=0, keepdims=True)
            scale = 1.0 / jnp.sqrt(energy * (1.0 / (SPAN * SPAN)) + 1.0)
            upd[band, s * wide:(s + 1) * wide] = field[s][band] * scale
    store_upd = pltpu.make_async_copy(upd, upd_hbm, sem.at[1])
    store_upd.start()
    store_new.wait()
    store_upd.wait()


def solution(mesh):
    nodes, chips = mesh.shape["node"], mesh.shape["chip"]

    def step(momentum, gradient, indices):
        _, rows, cols = momentum.shape
        spans, topk = indices.shape[1:]
        per = LANES // topk
        wide = per * SPAN
        used = 3 * (spans // per)
        cosines = jnp.asarray(cosine_blocks(per))
        hbm = pl.BlockSpec(memory_space=pltpu.HBM)
        vmem = pl.BlockSpec(memory_space=pltpu.VMEM)
        new_momentum, totals, tables = pl.pallas_call(
            functools.partial(kernel, nodes, chips, topk),
            out_shape=(
                pltpu.VMEM((rows, cols), F32),
                pltpu.VMEM((rows, cols), F32),
                pltpu.VMEM((4, wide, wide), BF16),
            ),
            in_specs=[hbm] * 4,
            out_specs=(vmem, vmem, vmem),
            scratch_shapes=[
                pltpu.VMEM((rows, cols), F32),
                pltpu.VMEM((rows, cols), BF16),
                pltpu.VMEM((spans, topk), jnp.int32),
                pltpu.VMEM((used, LANES), BF16),
                pltpu.VMEM((nodes * chips, used, LANES), BF16),
                pltpu.SemaphoreType.DMA((5,)),
                pltpu.SemaphoreType.DMA,
                pltpu.SemaphoreType.DMA((chips,)),
            ],
            compiler_params=pltpu.CompilerParams(
                collective_id=0, has_side_effects=True, vmem_limit_bytes=24 * 2**20
            ),
        )(*(pltpu.with_memory_space_constraint(x, pltpu.HBM) for x in (momentum, gradient, indices, cosines)))
        return tuple(pl.pallas_call(
            finish,
            out_shape=(
                jax.ShapeDtypeStruct((1, rows, cols), F32),
                jax.ShapeDtypeStruct((rows, cols), F32),
            ),
            in_specs=[vmem, vmem, vmem],
            out_specs=(hbm, hbm),
            scratch_shapes=[
                pltpu.VMEM((rows, cols), F32),
                pltpu.SemaphoreType.DMA((2,)),
            ],
            compiler_params=pltpu.CompilerParams(vmem_limit_bytes=24 * 2**20),
        )(new_momentum, totals, tables))

    return jax.shard_map(
        step,
        mesh=mesh,
        in_specs=(P(("node", "chip"), None, None),) * 3,
        out_specs=(P(("node", "chip"), None, None), P()),
        check_vma=False,
    )
```

```python
import functools
import math

import jax
import jax.numpy as jnp
import numpy as np
from jax import lax
from jax.experimental import pallas as pl
from jax.experimental.pallas import tpu as pltpu
from jax.sharding import PartitionSpec as P

SPAN = 64
LANES = 128
MESH = pl.DeviceIdType.MESH
F32 = jnp.float32
BF16 = jnp.bfloat16


def cosine_blocks(copies):
    orders = np.arange(SPAN, dtype=np.float64)
    wave, cell = orders[:, None], orders[None, :]
    factor = np.where(wave == 0, math.sqrt(1 / SPAN), math.sqrt(2 / SPAN))
    table = factor * np.cos(math.pi * (2 * cell + 1) * wave / (2 * SPAN))
    full = np.kron(np.eye(copies), table)
    high = full.astype(BF16)
    low = (full - high.astype(np.float64)).astype(BF16)
    return np.stack([high.T, low.T, high, low])


def halves(x):
    high = x.astype(BF16)
    return high, (x - high.astype(F32)).astype(BF16)


def mm(a, b):
    return lax.dot_general(a, b, (((1,), (0,)), ((), ())), preferred_element_type=F32)


def mm_nt(a, b):
    return lax.dot_general(a, b, (((1,), (1,)), ((), ())), preferred_element_type=F32)


def both_sides(blocks, left, right):
    outs = []
    for x in blocks:
        high, low = halves(x)
        y = mm(high, right[0]) + (mm(low, right[0]) + mm(high, right[1]))
        high, low = halves(y)
        outs.append(mm(left[0], high) + (mm(left[0], low) + mm(left[1], high)))
    return outs


def kernel(
    nodes, chips, topk, mom_hbm, grad_hbm, idx_hbm, cos_hbm, new_out, acc, cos,
    mom, grad, idx, box, recv, in_sem, send_sem, recv_sem,
):
    node, chip = lax.axis_index("node"), lax.axis_index("chip")
    count = nodes * chips
    rows, cols = mom.shape
    per = LANES // topk
    wide = per * SPAN
    groups = idx.shape[0] // per
    strips = cols // wide
    used = 3 * groups

    loads = [
        pltpu.make_async_copy(src, dst, in_sem.at[i])
        for i, (src, dst) in enumerate(
            (
                (idx_hbm.at[0], idx),
                (cos_hbm.at[pl.ds(0, 2)], cos.at[pl.ds(0, 2)]),
                (mom_hbm.at[0], mom),
                (grad_hbm.at[0], grad),
                (cos_hbm.at[pl.ds(2, 2)], cos.at[pl.ds(2, 2)]),
            )
        )
    ]
    for load in loads:
        load.start()

    barrier = pltpu.get_barrier_semaphore()

    high_side = 2 * chip >= chips
    half = nodes // 2 if nodes % 2 == 0 else nodes

    def plane(t):
        up = t + (chip <= t).astype(jnp.int32)
        down = chips - 1 - t
        return jnp.where(high_side, up, down - (down <= chip).astype(jnp.int32))

    def peers(visit):
        def one(to_chip, base, i):
            spot = base + i
            visit({"node": jnp.where(spot >= nodes, spot - nodes, spot), "chip": to_chip})

        for t in range(chips):
            own = t == chips - 1
            go = functools.partial(one, *((chip, node) if own else (plane(t), nodes - 1 - node)))
            if nodes <= 8:
                for i in range(1 if own else 0, nodes):
                    go(i)
            else:
                pl.loop(1 if own else 0, nodes)(go)

    peers(lambda to: pl.semaphore_signal(barrier, inc=1, device_id=to, device_id_type=MESH))

    loads[0].wait()
    slots = idx[...]
    spans = slots.shape[0]
    lane = lax.broadcasted_iota(jnp.int32, (spans, LANES), 1)
    place = lax.broadcasted_iota(jnp.int32, (spans, LANES), 0) % per
    spread = jnp.concatenate([slots] * per, axis=1)
    spread = jnp.where(lane // topk == place, spread + place * (SPAN * SPAN), 0)
    lists = [
        jnp.sum(spread[g * per:(g + 1) * per], axis=0, keepdims=True) for g in range(groups)
    ]
    wave = [(x // SPAN) % SPAN for x in lists]
    wide_pos = [(x // (SPAN * SPAN)) * SPAN + x % SPAN for x in lists]
    tall_iota = lax.broadcasted_iota(jnp.int32, (SPAN, LANES), 0)
    wide_iota = lax.broadcasted_iota(jnp.int32, (wide, LANES), 0)
    wave_hot = [(tall_iota == w).astype(F32).astype(BF16) for w in wave]
    wide_hot = [(wide_iota == w).astype(F32).astype(BF16) for w in wide_pos]

    loads[1].wait()
    tall_cos = [
        mm(cos[0, :SPAN, :SPAN], hot) + mm(cos[1, :SPAN, :SPAN], hot) for hot in wave_hot
    ]
    wide_high = [mm(cos[0], hot).astype(BF16) for hot in wide_hot]
    wide_low = [mm(cos[1], hot).astype(BF16) for hot in wide_hot]

    loads[2].wait()
    loads[3].wait()
    blended = 0.9 * mom[...] + grad[...].astype(F32)

    def part(g):
        a, s = g // strips, g % strips
        return a, s

    def region(g):
        a, s = part(g)
        return slice(a * SPAN, (a + 1) * SPAN), slice(s * wide, (s + 1) * wide)

    picked = []
    for g in range(groups):
        high, low = halves(blended[region(g)])
        sums = mm(high, wide_high[g]) + (mm(low, wide_high[g]) + mm(high, wide_low[g]))
        picked.append(jnp.sum(sums * tall_cos[g], axis=0, keepdims=True))
    payload = jnp.concatenate(
        picked + [w.astype(F32) for w in wave] + [w.astype(F32) for w in wide_pos], axis=0
    ).astype(BF16)
    me = chip * nodes + node
    box[...] = payload
    recv[me] = payload

    pl.semaphore_wait(barrier, count - 1)
    peers(
        lambda to: pltpu.make_async_remote_copy(
            src_ref=box,
            dst_ref=recv.at[me],
            send_sem=send_sem,
            recv_sem=recv_sem.at[chip, node // half],
            device_id=to,
            device_id_type=MESH,
        ).start()
    )

    for g in range(groups):
        sent_value = picked[g].astype(BF16).astype(F32)
        high, low = halves(tall_cos[g] * sent_value)
        own_part = mm_nt(high, wide_high[g]) + (
            mm_nt(low, wide_high[g]) + mm_nt(high, wide_low[g])
        )
        new_out[region(g)] = blended[region(g)] - own_part

    acc[...] = jnp.zeros_like(acc)
    batch = math.gcd(half, 8)

    def decode(start):
        block = recv[pl.ds(start, batch)].astype(F32)
        for g in range(groups):
            left, right = [], []
            for i in range(batch):
                val = block[i, g:g + 1]
                row = block[i, groups + g:groups + g + 1].astype(jnp.int32)
                col = block[i, 2 * groups + g:2 * groups + g + 1].astype(jnp.int32)
                left.append(jnp.where(tall_iota == row, val, 0.0).astype(BF16))
                right.append((wide_iota == col).astype(F32).astype(BF16))
            a, s = part(g)
            acc[pl.ds(a * SPAN, SPAN), pl.ds(s * wide, wide)] += mm_nt(
                jnp.concatenate(left, axis=1), jnp.concatenate(right, axis=1)
            )

    for t in reversed(range(chips)):
        source = chip if t == chips - 1 else plane(t)
        for h in range(nodes // half):
            part_no = lax.rem(node // half + h, nodes // half)
            first = source * nodes + part_no * half
            own = t == chips - 1 and h == 0
            if not (own and half == 1):
                landed = recv.at[pl.ds(first, half - 1 if own else half)]
                pltpu.make_async_copy(landed, landed, recv_sem.at[source, part_no]).wait()
            if half == batch:
                decode(first)
            else:
                pl.loop(0, half // batch)(lambda i: decode(first + i * batch))

    loads[4].wait()
    sent = recv.at[pl.ds(0, count - 1)]
    pltpu.make_async_copy(sent, sent, send_sem).wait()


def finish(new_in, acc, cos, new_hbm, upd_hbm, upd, sem):
    store_new = pltpu.make_async_copy(new_in, new_hbm.at[0], sem.at[0])
    store_new.start()
    rows, cols = acc.shape
    wide = cos.shape[-1]
    strips = cols // wide
    totals = [acc[:, s * wide:(s + 1) * wide] for s in range(strips)]
    same = (
        lax.broadcasted_iota(jnp.int32, (wide, wide), 0) // SPAN
        == lax.broadcasted_iota(jnp.int32, (wide, wide), 1) // SPAN
    ).astype(F32).astype(BF16)
    left = (cos[0, :rows, :rows], cos[1, :rows, :rows])
    stores = [store_new]
    for s in range(strips):
        scales = []
        for a in range(rows // SPAN):
            power = totals[s][a * SPAN:(a + 1) * SPAN]
            power = jnp.sum((power * power).reshape(SPAN // 8, 8, wide), axis=0)
            high, low = halves(power)
            energy = jnp.sum(mm(high, same) + mm(low, same), axis=0, keepdims=True)
            scales.append(1.0 / jnp.sqrt(energy * (1.0 / (SPAN * SPAN)) + 1.0))
        field = both_sides([totals[s]], left, (cos[2], cos[3]))[0]
        cut = pl.ds(s * wide, wide)
        for a, scale in enumerate(scales):
            band = slice(a * SPAN, (a + 1) * SPAN)
            upd[band, s * wide:(s + 1) * wide] = field[band] * scale
        store = pltpu.make_async_copy(upd.at[:, cut], upd_hbm.at[:, cut], sem.at[1 + s])
        store.start()
        stores.append(store)
    for store in stores:
        store.wait()


def solution(mesh):
    nodes, chips = mesh.shape["node"], mesh.shape["chip"]

    def step(momentum, gradient, indices):
        _, rows, cols = momentum.shape
        spans, topk = indices.shape[1:]
        per = LANES // topk
        wide = per * SPAN
        used = 3 * (spans // per)
        cosines = jnp.asarray(cosine_blocks(per))
        hbm = pl.BlockSpec(memory_space=pltpu.HBM)
        vmem = pl.BlockSpec(memory_space=pltpu.VMEM)
        new_momentum, totals, tables = pl.pallas_call(
            functools.partial(kernel, nodes, chips, topk),
            out_shape=(
                pltpu.VMEM((rows, cols), F32),
                pltpu.VMEM((rows, cols), F32),
                pltpu.VMEM((4, wide, wide), BF16),
            ),
            in_specs=[hbm] * 4,
            out_specs=(vmem, vmem, vmem),
            scratch_shapes=[
                pltpu.VMEM((rows, cols), F32),
                pltpu.VMEM((rows, cols), BF16),
                pltpu.VMEM((spans, topk), jnp.int32),
                pltpu.VMEM((used, LANES), BF16),
                pltpu.VMEM((nodes * chips, used, LANES), BF16),
                pltpu.SemaphoreType.DMA((5,)),
                pltpu.SemaphoreType.DMA,
                pltpu.SemaphoreType.DMA((chips, 2)),
            ],
            compiler_params=pltpu.CompilerParams(
                collective_id=0, has_side_effects=True, vmem_limit_bytes=24 * 2**20
            ),
        )(*(pltpu.with_memory_space_constraint(x, pltpu.HBM) for x in (momentum, gradient, indices, cosines)))
        return tuple(pl.pallas_call(
            finish,
            out_shape=(
                jax.ShapeDtypeStruct((1, rows, cols), F32),
                jax.ShapeDtypeStruct((rows, cols), F32),
            ),
            in_specs=[vmem, vmem, vmem],
            out_specs=(hbm, hbm),
            scratch_shapes=[
                pltpu.VMEM((rows, cols), F32),
                pltpu.SemaphoreType.DMA((1 + cols // wide,)),
            ],
            compiler_params=pltpu.CompilerParams(vmem_limit_bytes=24 * 2**20),
        )(new_momentum, totals, tables))

    return jax.shard_map(
        step,
        mesh=mesh,
        in_specs=(P(("node", "chip"), None, None),) * 3,
        out_specs=(P(("node", "chip"), None, None), P()),
        check_vma=False,
    )
```

```python
import functools
import math

import jax
import jax.numpy as jnp
import numpy as np
from jax import lax
from jax.experimental import pallas as pl
from jax.experimental.pallas import tpu as pltpu
from jax.sharding import PartitionSpec as P

SPAN = 64
LANES = 128
MESH = pl.DeviceIdType.MESH
F32 = jnp.float32
BF16 = jnp.bfloat16


def cosine_blocks(copies):
    orders = np.arange(SPAN, dtype=np.float64)
    wave, cell = orders[:, None], orders[None, :]
    factor = np.where(wave == 0, math.sqrt(1 / SPAN), math.sqrt(2 / SPAN))
    table = factor * np.cos(math.pi * (2 * cell + 1) * wave / (2 * SPAN))
    full = np.kron(np.eye(copies), table)
    high = full.astype(BF16)
    low = (full - high.astype(np.float64)).astype(BF16)
    return np.stack([high.T, low.T, high, low])


def halves(x):
    high = x.astype(BF16)
    return high, (x - high.astype(F32)).astype(BF16)


def mm(a, b):
    return lax.dot_general(a, b, (((1,), (0,)), ((), ())), preferred_element_type=F32)


def mm_nt(a, b):
    return lax.dot_general(a, b, (((1,), (1,)), ((), ())), preferred_element_type=F32)


def both_sides(blocks, left, right):
    outs = []
    for x in blocks:
        high, low = halves(x)
        y = mm(high, right[0]) + (mm(low, right[0]) + mm(high, right[1]))
        high, low = halves(y)
        outs.append(mm(left[0], high) + (mm(left[0], low) + mm(left[1], high)))
    return outs


def kernel(
    nodes, chips, topk, mom_hbm, grad_hbm, idx_hbm, cos_hbm, new_out, acc, cos,
    mom, grad, idx, box, recv, in_sem, send_sem, recv_sem,
):
    node, chip = lax.axis_index("node"), lax.axis_index("chip")
    count = nodes * chips
    rows, cols = mom.shape
    per = LANES // topk
    wide = per * SPAN
    groups = idx.shape[0] // per
    strips = cols // wide
    used = 3 * groups

    loads = [
        pltpu.make_async_copy(src, dst, in_sem.at[i])
        for i, (src, dst) in enumerate(
            (
                (idx_hbm.at[0], idx),
                (cos_hbm.at[pl.ds(0, 2)], cos.at[pl.ds(0, 2)]),
                (mom_hbm.at[0], mom),
                (grad_hbm.at[0], grad),
                (cos_hbm.at[pl.ds(2, 2)], cos.at[pl.ds(2, 2)]),
            )
        )
    ]
    for load in loads:
        load.start()

    barrier = pltpu.get_barrier_semaphore()

    high_side = 2 * chip >= chips
    half = nodes // 2 if nodes % 2 == 0 else nodes

    def plane(t):
        up = t + (chip <= t).astype(jnp.int32)
        down = chips - 1 - t
        return jnp.where(high_side, up, down - (down <= chip).astype(jnp.int32))

    def peers(visit):
        def one(to_chip, base, i):
            spot = base + i
            visit({"node": jnp.where(spot >= nodes, spot - nodes, spot), "chip": to_chip})

        for t in range(chips):
            own = t == chips - 1
            go = functools.partial(one, *((chip, node) if own else (plane(t), nodes - 1 - node)))
            if nodes <= 8:
                for i in range(1 if own else 0, nodes):
                    go(i)
            else:
                pl.loop(1 if own else 0, nodes)(go)

    peers(lambda to: pl.semaphore_signal(barrier, inc=1, device_id=to, device_id_type=MESH))

    loads[0].wait()
    slots = idx[...]
    spans = slots.shape[0]
    lane = lax.broadcasted_iota(jnp.int32, (spans, LANES), 1)
    place = lax.broadcasted_iota(jnp.int32, (spans, LANES), 0) % per
    spread = jnp.concatenate([slots] * per, axis=1)
    spread = jnp.where(lane // topk == place, spread + place * (SPAN * SPAN), 0)
    lists = [
        jnp.sum(spread[g * per:(g + 1) * per], axis=0, keepdims=True) for g in range(groups)
    ]
    wave = [(x // SPAN) % SPAN for x in lists]
    wide_pos = [(x // (SPAN * SPAN)) * SPAN + x % SPAN for x in lists]
    tall_iota = lax.broadcasted_iota(jnp.int32, (SPAN, LANES), 0)
    wide_iota = lax.broadcasted_iota(jnp.int32, (wide, LANES), 0)
    wave_hot = [(tall_iota == w).astype(F32).astype(BF16) for w in wave]
    wide_hot = [(wide_iota == w).astype(F32).astype(BF16) for w in wide_pos]

    loads[1].wait()
    tall_cos = [
        mm(cos[0, :SPAN, :SPAN], hot) + mm(cos[1, :SPAN, :SPAN], hot) for hot in wave_hot
    ]
    edge = cos.shape[-1]

    def columns(table, hot):
        pieces = [mm(table, hot[p:p + edge]).astype(BF16) for p in range(0, wide, edge)]
        return jnp.concatenate(pieces, axis=0)

    wide_high = [columns(cos[0], hot) for hot in wide_hot]
    wide_low = [columns(cos[1], hot) for hot in wide_hot]

    loads[2].wait()
    loads[3].wait()
    blended = 0.9 * mom[...] + grad[...].astype(F32)

    def part(g):
        a, s = g // strips, g % strips
        return a, s

    def region(g):
        a, s = part(g)
        return slice(a * SPAN, (a + 1) * SPAN), slice(s * wide, (s + 1) * wide)

    picked = []
    for g in range(groups):
        high, low = halves(blended[region(g)])
        sums = mm(high, wide_high[g]) + (mm(low, wide_high[g]) + mm(high, wide_low[g]))
        picked.append(jnp.sum(sums * tall_cos[g], axis=0, keepdims=True))
    payload = jnp.concatenate(
        picked + [w.astype(F32) for w in wave] + [w.astype(F32) for w in wide_pos], axis=0
    ).astype(BF16)
    me = chip * nodes + node
    box[...] = payload
    recv[me] = payload

    pl.semaphore_wait(barrier, count - 1)
    peers(
        lambda to: pltpu.make_async_remote_copy(
            src_ref=box,
            dst_ref=recv.at[me],
            send_sem=send_sem,
            recv_sem=recv_sem.at[chip, node // half],
            device_id=to,
            device_id_type=MESH,
        ).start()
    )

    for g in range(groups):
        sent_value = picked[g].astype(BF16).astype(F32)
        high, low = halves(tall_cos[g] * sent_value)
        own_part = mm_nt(high, wide_high[g]) + (
            mm_nt(low, wide_high[g]) + mm_nt(high, wide_low[g])
        )
        new_out[region(g)] = blended[region(g)] - own_part

    acc[...] = jnp.zeros_like(acc)
    batch = math.gcd(half, 8)

    def decode(start):
        block = recv[pl.ds(start, batch)].astype(F32)
        for g in range(groups):
            left, right = [], []
            for i in range(batch):
                val = block[i, g:g + 1]
                row = block[i, groups + g:groups + g + 1].astype(jnp.int32)
                col = block[i, 2 * groups + g:2 * groups + g + 1].astype(jnp.int32)
                left.append(jnp.where(tall_iota == row, val, 0.0).astype(BF16))
                right.append((wide_iota == col).astype(F32).astype(BF16))
            a, s = part(g)
            acc[pl.ds(a * SPAN, SPAN), pl.ds(s * wide, wide)] += mm_nt(
                jnp.concatenate(left, axis=1), jnp.concatenate(right, axis=1)
            )

    for t in reversed(range(chips)):
        source = chip if t == chips - 1 else plane(t)
        for h in range(nodes // half):
            part_no = lax.rem(node // half + h, nodes // half)
            first = source * nodes + part_no * half
            own = t == chips - 1 and h == 0
            if not (own and half == 1):
                landed = recv.at[pl.ds(first, half - 1 if own else half)]
                pltpu.make_async_copy(landed, landed, recv_sem.at[source, part_no]).wait()
            if half == batch:
                decode(first)
            else:
                pl.loop(0, half // batch)(lambda i: decode(first + i * batch))

    loads[4].wait()
    sent = recv.at[pl.ds(0, count - 1)]
    pltpu.make_async_copy(sent, sent, send_sem).wait()


def finish(new_in, acc, cos, new_hbm, upd_hbm, upd, sem):
    store_new = pltpu.make_async_copy(new_in, new_hbm.at[0], sem.at[0])
    store_new.start()
    rows, cols = acc.shape
    wide = cos.shape[-1]
    strips = cols // wide
    totals = [acc[:, s * wide:(s + 1) * wide] for s in range(strips)]
    same = (
        lax.broadcasted_iota(jnp.int32, (wide, wide), 0) // SPAN
        == lax.broadcasted_iota(jnp.int32, (wide, wide), 1) // SPAN
    ).astype(F32).astype(BF16)
    left = (cos[0, :rows, :rows], cos[1, :rows, :rows])
    stores = [store_new]
    for s in range(strips):
        scales = []
        for a in range(rows // SPAN):
            power = totals[s][a * SPAN:(a + 1) * SPAN]
            power = jnp.sum((power * power).reshape(SPAN // 8, 8, wide), axis=0)
            high, low = halves(power)
            energy = jnp.sum(mm(high, same) + mm(low, same), axis=0, keepdims=True)
            scales.append(1.0 / jnp.sqrt(energy * (1.0 / (SPAN * SPAN)) + 1.0))
        field = both_sides([totals[s]], left, (cos[2], cos[3]))[0]
        cut = pl.ds(s * wide, wide)
        for a, scale in enumerate(scales):
            band = slice(a * SPAN, (a + 1) * SPAN)
            upd[band, s * wide:(s + 1) * wide] = field[band] * scale
        store = pltpu.make_async_copy(upd.at[:, cut], upd_hbm.at[:, cut], sem.at[1 + s])
        store.start()
        stores.append(store)
    for store in stores:
        store.wait()


def solution(mesh):
    nodes, chips = mesh.shape["node"], mesh.shape["chip"]

    def step(momentum, gradient, indices):
        _, rows, cols = momentum.shape
        spans, topk = indices.shape[1:]
        per = LANES // topk
        wide = per * SPAN
        used = 3 * (spans // per)
        cosines = jnp.asarray(cosine_blocks(2))
        hbm = pl.BlockSpec(memory_space=pltpu.HBM)
        vmem = pl.BlockSpec(memory_space=pltpu.VMEM)
        new_momentum, totals, tables = pl.pallas_call(
            functools.partial(kernel, nodes, chips, topk),
            out_shape=(
                pltpu.VMEM((rows, cols), F32),
                pltpu.VMEM((rows, cols), F32),
                pltpu.VMEM((4, 2 * SPAN, 2 * SPAN), BF16),
            ),
            in_specs=[hbm] * 4,
            out_specs=(vmem, vmem, vmem),
            scratch_shapes=[
                pltpu.VMEM((rows, cols), F32),
                pltpu.VMEM((rows, cols), BF16),
                pltpu.VMEM((spans, topk), jnp.int32),
                pltpu.VMEM((used, LANES), BF16),
                pltpu.VMEM((nodes * chips, used, LANES), BF16),
                pltpu.SemaphoreType.DMA((5,)),
                pltpu.SemaphoreType.DMA,
                pltpu.SemaphoreType.DMA((chips, 2)),
            ],
            compiler_params=pltpu.CompilerParams(
                collective_id=0, has_side_effects=True, vmem_limit_bytes=24 * 2**20
            ),
        )(*(pltpu.with_memory_space_constraint(x, pltpu.HBM) for x in (momentum, gradient, indices, cosines)))
        return tuple(pl.pallas_call(
            finish,
            out_shape=(
                jax.ShapeDtypeStruct((1, rows, cols), F32),
                jax.ShapeDtypeStruct((rows, cols), F32),
            ),
            in_specs=[vmem, vmem, vmem],
            out_specs=(hbm, hbm),
            scratch_shapes=[
                pltpu.VMEM((rows, cols), F32),
                pltpu.SemaphoreType.DMA((1 + cols // (2 * SPAN),)),
            ],
            compiler_params=pltpu.CompilerParams(vmem_limit_bytes=24 * 2**20),
        )(new_momentum, totals, tables))

    return jax.shard_map(
        step,
        mesh=mesh,
        in_specs=(P(("node", "chip"), None, None),) * 3,
        out_specs=(P(("node", "chip"), None, None), P()),
        check_vma=False,
    )
```
